32 devices in a mesh: egrp: 8 (over y, x, core), eloc: 4 (over z).
Axes of the slice: x: 2, y: 2, z: 4, core: 2. Of those that a mesh axis runs over, the one named last changes fastest.
Arguments:
- green_blocks: bfloat16 [32, 16, 3, 64, 128], P(('egrp', 'eloc')), may hold values from -0.3125 to 0.3125
- sigma_prev: bfloat16 [32, 16, 64, 128], P(('egrp', 'eloc')), may hold values from -6 to 6
- neighbours: int32 [16, 2], replicated, may hold values from 0 to 15
- couplings: bfloat16 [6, 16, 64, 128], P(None, 'eloc'), may hold values from -0.375 to 0.375
- occupancy: float32 [6], replicated, may hold values from 0.1 to 2
- shifts: int32 [6], replicated, may hold values from 1 to 4, as said below
Outputs:
- sigma_next: bfloat16 [32, 16, 64, 128], P(('egrp', 'eloc'))
The draws below stay inside these ranges and needn't reach their ends.
Inputs may be any that keep to these rules, and one draw needn't show every extreme that they name: `shifts`: at least one mode's shift equals 4.
All inputs are finite; a program needn't handle non-finite values.
Results may differ from the reference program's by a relative error of at most 0.0065.
Values may be sent and summed in bfloat16 or wider, within the bound.
No kernel may reach another device: no remote copies, remote signals or barrier semaphores. Data moves between devices by JAX's collectives and lax.ppermute only.
A program may use at most 64 MiB of HBM per device.

```python
import math
import jax
import jax.numpy as jnp
from jax import lax

ORB = 64
ATOMS = 16
MODES = 6
GROUP = 4
ENERGIES = 32


def draw_shifts(key, part):
    first_key, second_key = jax.random.split(jax.random.fold_in(key, 11))
    drawn = jax.random.randint(first_key, (MODES,), 1, GROUP + 1)
    picked = jax.random.randint(second_key, (), 0, MODES)
    return jnp.where(jnp.arange(MODES) == picked, GROUP, drawn).astype(jnp.int32)


def plant(values, stream_key, low, largest):
    longest = values.shape.index(max(values.shape))
    spots = []
    for shift in (0, 1):
        where = [jax.random.randint(jax.random.fold_in(stream_key, axis), (), 0, length) for axis, length in enumerate(values.shape)]
        where[longest] = (where[longest] + shift) % values.shape[longest]
        spots.append(tuple(where))
    return values.at[spots[0]].set(low).at[spots[1]].set(largest)


def steps_of(stream_key, extent, shards, least, largest):
    def one(dim, parts):
        draws = jax.random.uniform(jax.random.fold_in(jax.random.fold_in(stream_key, 6), dim), (parts,), jnp.float32, least / len(shards), largest / len(shards))
        return jnp.repeat(jnp.exp(draws), extent[dim] // parts).reshape((-1,) + (1,) * (len(extent) - dim - 1))

    factor_of = one(*shards[0])
    for cut in shards[1:]:
        factor_of = factor_of * one(*cut)
    return factor_of


def scatter_about(own_key, dims, width, bound, pieces=(), kind=jnp.bfloat16):
    entries = jax.random.normal(own_key, dims, jnp.float32) * width
    if len(pieces) > 0:
        entries = steps_of(own_key, dims, pieces, -0.22, 0.18) * entries
    return jnp.clip(entries, min=-bound, max=bound).astype(kind)


def setup_inputs(seed: int = 0) -> dict:
    streams_of = jax.random.split(jax.random.key(seed), 7)
    green_blocks = scatter_about(streams_of[0], (ENERGIES, ATOMS, 3, ORB, 2 * ORB), (6 * ORB) ** -0.5, 0.3125, ((0, 32),))
    sigma_prev = scatter_about(streams_of[1], (ENERGIES, ATOMS, ORB, 2 * ORB), 1.0, 6.0, ((0, 32),))
    neighbours = plant(jax.random.randint(streams_of[2], (ATOMS, 2), 0, ATOMS), jax.random.fold_in(streams_of[2], 1), 0, ATOMS - 1).astype(jnp.int32)
    couplings = scatter_about(streams_of[3], (MODES, ATOMS, ORB, 2 * ORB), (4 * ORB) ** -0.5, 0.375, ((1, 4),))
    occupancy = jnp.clip(jnp.exp(jax.random.uniform(streams_of[4], (MODES,), jnp.float32, math.log(0.1), math.log(2.0))), 0.1, 2.0)
    shifts = draw_shifts(jax.random.fold_in(streams_of[6], 71), 0)
    return {"green_blocks": green_blocks, "sigma_prev": sigma_prev, "neighbours": neighbours, "couplings": couplings, "occupancy": occupancy, "shifts": shifts}


def widened_form(block):
    orbitals = block.shape[-2]
    real_part = block[..., :orbitals]
    imag_part = block[..., orbitals:]
    upper_rows = jnp.concatenate([real_part, imag_part], -1)
    lower_rows = jnp.concatenate([-imag_part, real_part], -1)
    return jnp.concatenate([upper_rows, lower_rows], -2)


def adjoint_form(block):
    orbitals = block.shape[-2]
    real_part = jnp.swapaxes(block[..., :orbitals], -1, -2)
    imag_part = jnp.swapaxes(block[..., orbitals:], -1, -2)
    upper_rows = jnp.concatenate([real_part, -imag_part], -1)
    lower_rows = jnp.concatenate([imag_part, real_part], -1)
    return jnp.concatenate([upper_rows, lower_rows], -2)


def reference(green_blocks, sigma_prev, neighbours, couplings, occupancy, shifts):
    atom_index = jnp.concatenate([jnp.arange(ATOMS, dtype=jnp.int32)[:, None], neighbours.astype(jnp.int32)], 1)

    def lesser_one(operands):
        blocks, sigma_local = operands
        chosen = sigma_local[atom_index]
        half_product = jnp.einsum('akij,akjl->akil', blocks.astype(jnp.float32), widened_form(chosen).astype(jnp.float32)).astype(jnp.bfloat16)
        return jnp.einsum('akij,akjl->ail', half_product.astype(jnp.float32), adjoint_form(blocks).astype(jnp.float32))

    lesser = lax.map(lesser_one, (green_blocks, sigma_prev))

    def sigma_atom(operands):
        column, coupling = operands
        padding = jnp.zeros((GROUP,) + column.shape[1:], jnp.float32)
        padded = jnp.concatenate([padding, column, padding], 0)
        accumulated = jnp.zeros(column.shape, jnp.float32)
        for mode_index in range(MODES):
            shift_now = shifts[mode_index].astype(jnp.int32)
            upper_part = lax.dynamic_slice_in_dim(padded, (GROUP + shift_now).astype(jnp.int32), ENERGIES, 0)
            lower_part = lax.dynamic_slice_in_dim(padded, (GROUP - shift_now).astype(jnp.int32), ENERGIES, 0)
            mixture = (occupancy[mode_index] + 1.0) * upper_part + occupancy[mode_index] * lower_part
            coupling_float = coupling[mode_index].astype(jnp.float32)
            left = jnp.einsum('ij,ejl->eil', coupling_float, widened_form(mixture), precision=lax.Precision.HIGHEST)
            accumulated = accumulated + jnp.einsum('eij,jl->eil', left, adjoint_form(coupling_float), precision=lax.Precision.HIGHEST)
        return accumulated

    by_atom = lax.map(sigma_atom, (jnp.moveaxis(lesser, 1, 0), jnp.moveaxis(couplings, 1, 0)))
    return jnp.moveaxis(by_atom, 0, 1).astype(jnp.bfloat16)
```

```python
import jax
import jax.numpy as jnp
from jax import lax
from jax.experimental import pallas as pl
from jax.experimental.pallas import tpu as pltpu
from jax.sharding import PartitionSpec as P

VMEM = pl.BlockSpec(memory_space=pltpu.VMEM)
SMEM = pl.BlockSpec(memory_space=pltpu.SMEM)
BF16 = jnp.bfloat16
NT = (((1,), (1,)), ((), ()))


def partner(i, k, n):
    return i ^ k if n & (n - 1) == 0 else (i + k) % n


def source(i, k, n):
    return i ^ k if n & (n - 1) == 0 else (i + n - k) % n


def slot_of(i, j, n):
    return i ^ j if n & (n - 1) == 0 else lax.rem(i - j + n, n)


def target_at(me, k, n):
    return me ^ k if n & (n - 1) == 0 else lax.rem(me + k, n)


def source_at(me, k, n):
    return me ^ k if n & (n - 1) == 0 else lax.rem(me + n - k, n)


def turned(block):
    half = block.shape[-1] // 2
    return jnp.concatenate([-block[:, half:], block[:, :half]], -1)


def lesser_kernel(n, ks, neighbours, green, sigma, *outs):
    me = lax.axis_index("eloc")
    per = outs[0].shape[0]
    for k, out in zip(ks, outs):
        base = target_at(me, k, n) * per
        for i in range(per):
            atom = base + i
            halves, uppers, lowers = [], [], []
            for j in range(green.shape[2]):
                block = green[0, atom, j]
                other = atom if j == 0 else neighbours[atom, j - 1]
                chosen = sigma[0, other]
                wide = jnp.concatenate([chosen, turned(chosen)], 0)
                half = jnp.dot(block, wide, preferred_element_type=jnp.float32)
                halves.append(half.astype(BF16))
                uppers.append(block)
                lowers.append(turned(block))
            left = jnp.concatenate(halves, 1)
            right = jnp.concatenate([jnp.concatenate(uppers, 1), jnp.concatenate(lowers, 1)], 0)
            total = lax.dot_general(left, right, NT, preferred_element_type=jnp.float32)
            out[i] = total.astype(BF16)


def lesser_blocks(n, per, ks, neighbours, green, sigma):
    orb = sigma.shape[-2]

    def kernel(*refs):
        lesser_kernel(n, ks, *refs)

    return pl.pallas_call(
        kernel,
        name="lesser",
        out_shape=[jax.ShapeDtypeStruct((per, orb, 2 * orb), BF16) for _ in ks],
        in_specs=[SMEM, VMEM, VMEM],
        out_specs=[VMEM for _ in ks],
        cost_estimate=pl.CostEstimate(flops=400_000_000, bytes_accessed=2_000_000, transcendentals=0),
    )(neighbours, green, sigma)


def prepare_kernel(occupancy, couplings, right, left):
    modes, per, orb, _ = couplings.shape
    for a in range(per):
        for m in range(modes):
            block = couplings[m, a]
            wide = jnp.concatenate([block, turned(block)], 0).astype(jnp.float32)
            occ = occupancy[m]
            right[a, m, :, : 2 * orb] = (wide * (occ + 1.0)).astype(BF16)
            right[a, m, :, 2 * orb :] = (wide * occ).astype(BF16)
        left[a, :orb] = jnp.concatenate([couplings[m, a][:, :orb] for m in range(modes)], 1)
        left[a, orb:] = jnp.concatenate([couplings[m, a][:, orb:] for m in range(modes)], 1)


def prepared(occupancy, couplings):
    modes, per, orb, _ = couplings.shape
    return pl.pallas_call(
        prepare_kernel,
        name="prepare",
        out_shape=[
            jax.ShapeDtypeStruct((per, modes, 2 * orb, 4 * orb), BF16),
            jax.ShapeDtypeStruct((per, 2 * orb, modes * orb), BF16),
        ],
        in_specs=[SMEM, VMEM],
        out_specs=[VMEM, VMEM],
        cost_estimate=pl.CostEstimate(flops=200_000_000, bytes_accessed=2_000_000, transcendentals=0),
    )(occupancy, couplings)


def modes_kernel(n, ks, shifts, before, here, after, right, left, *rest):
    outs, stack = rest[: len(ks)], rest[-1]
    me = lax.axis_index("eloc")
    per, orb = outs[0].shape[0], outs[0].shape[1]
    modes = right.shape[1]
    width = 2 if len(ks) % 2 == 0 else 1

    def row(t, a):
        slot = slot_of(me, lax.rem(t + n, n), n)
        return slot, t

    for a in range(per):
        for m in range(modes):
            shift = shifts[m]
            rows = []
            for k in ks:
                e = target_at(me, k, n)
                pieces = []
                for t in (e + shift + n, e - shift + n):
                    place = (t // n) * n + slot_of(me, lax.rem(t, n), n)
                    pieces.append(here[place, a])
                rows.append(jnp.concatenate(pieces, 1))
            stacked = jnp.concatenate(rows, 0)
            product = lax.dot_general(stacked, right[a, m], NT, preferred_element_type=jnp.float32)
            product = product.astype(BF16)
            for q in range(len(ks)):
                stack[a, q // width, m * orb : (m + 1) * orb, (q % width) * 2 * orb : (q % width + 1) * 2 * orb] = (
                    product[q * orb : (q + 1) * orb]
                )
        for p in range(len(ks) // width):
            both = jnp.dot(left[a], stack[a, p], preferred_element_type=jnp.float32)
            for w in range(width):
                piece = both[:, w * 2 * orb : (w + 1) * 2 * orb]
                outs[p * width + w][a] = (piece[:orb] + turned(piece[orb:])).astype(BF16)


def mode_blocks(n, ks, shifts, extended, right, left):
    per, modes, wide, _ = right.shape
    orb = wide // 2
    width = 2 if len(ks) % 2 == 0 else 1

    def kernel(shifts, here, right, left, *rest):
        modes_kernel(n, ks, shifts, None, here, None, right, left, *rest)

    return pl.pallas_call(
        kernel,
        name="modes",
        out_shape=[jax.ShapeDtypeStruct((per, orb, 2 * orb), BF16) for _ in ks],
        in_specs=[SMEM, VMEM, VMEM, VMEM],
        out_specs=[VMEM for _ in ks],
        scratch_shapes=[pltpu.VMEM((per, len(ks) // width, modes * orb, width * 2 * orb), BF16)],
        cost_estimate=pl.CostEstimate(flops=400_000_000, bytes_accessed=2_000_000, transcendentals=0),
    )(shifts, extended, right, left)


def join_kernel(n, *refs):
    out = refs[-1]
    me = lax.axis_index("eloc")
    per = refs[0].shape[0]
    for k in range(n):
        out[0, pl.ds(source_at(me, k, n) * per, per)] = refs[k][...]


def joined(n, blocks):
    per, orb, wide = blocks[0].shape

    def kernel(*refs):
        join_kernel(n, *refs)

    return pl.pallas_call(
        kernel,
        name="join",
        out_shape=jax.ShapeDtypeStruct((1, n * per, orb, wide), BF16),
        in_specs=[VMEM for _ in blocks],
        out_specs=VMEM,
    )(*blocks)


def exchanged(n, blocks):
    return [blocks[0]] + [
        lax.ppermute(blocks[k], "eloc", [(i, partner(i, k, n)) for i in range(n)]) for k in range(1, n)
    ]


def shards(green_blocks, sigma_prev, neighbours, couplings, occupancy, shifts):
    n, groups = lax.axis_size("eloc"), lax.axis_size("egrp")
    per = couplings.shape[1]
    ks = tuple(range(n))
    sent = lesser_blocks(n, per, ks, neighbours, green_blocks, sigma_prev)
    right, left = prepared(occupancy, couplings)
    here = jnp.stack(exchanged(n, sent))
    before = lax.ppermute(here, "egrp", [(i, i + 1) for i in range(groups - 1)])
    after = lax.ppermute(here, "egrp", [(i + 1, i) for i in range(groups - 1)])
    extended = jnp.concatenate([before, here, after], 0)
    results = mode_blocks(n, ks, shifts, extended, right, left)
    return joined(n, exchanged(n, results))


def solution(mesh):
    return jax.shard_map(
        shards,
        mesh=mesh,
        in_specs=(
            P(("egrp", "eloc"), None, None, None, None),
            P(("egrp", "eloc"), None, None, None),
            P(),
            P(None, "eloc", None, None),
            P(),
            P(),
        ),
        out_specs=P(("egrp", "eloc"), None, None, None),
        check_vma=False,
    )
```

```python
import jax
import jax.numpy as jnp
from jax import lax
from jax.experimental import pallas as pl
from jax.experimental.pallas import tpu as pltpu
from jax.sharding import PartitionSpec as P


VMEM = pl.BlockSpec(memory_space=pltpu.VMEM)
SMEM = pl.BlockSpec(memory_space=pltpu.SMEM)
HBM = pl.BlockSpec(memory_space=pltpu.HBM)
BF16 = jnp.bfloat16
F32 = jnp.float32
NT = (((1,), (1,)), ((), ()))


def limited():
    return pltpu.CompilerParams(vmem_limit_bytes=12 * 1024 * 1024)


def cost(flops):
    return pl.CostEstimate(flops=flops, bytes_accessed=1_000_000, transcendentals=0)


def two_power(n):
    return n & (n - 1) == 0


def partner(i, k, n):
    return i ^ k if two_power(n) else (i + k) % n


def target_at(me, k, n):
    return me ^ k if two_power(n) else lax.rem(me + k, n)


def source_at(me, k, n):
    return me ^ k if two_power(n) else lax.rem(me + n - k, n)


def place_of(me, t, n):
    if two_power(n):
        return (t & ~(n - 1)) + (me ^ (t & (n - 1)))
    inside = lax.rem(t, n)
    return t - inside + lax.rem(me - inside + n, n)


def turned(block):
    half = block.shape[-1] // 2
    return jnp.concatenate([-block[:, half:], block[:, :half]], -1)


def widened(block):
    return jnp.concatenate([block, turned(block)], 0)


def lesser_of(blocks, chosen):
    total = None
    for block, other in zip(blocks, chosen):
        half = jnp.dot(block, widened(other), preferred_element_type=F32).astype(BF16)
        term = lax.dot_general(half, widened(block), NT, preferred_element_type=F32)
        total = term if total is None else total + term
    return total.astype(BF16)


def opened():
    def kernel(out):
        out[...] = jnp.zeros_like(out)

    return pl.pallas_call(
        kernel,
        name="opening",
        out_shape=jax.ShapeDtypeStruct((8, 128), jnp.int32),
        out_specs=VMEM,
        compiler_params=limited(),
        cost_estimate=cost(4_000_000_000),
    )()


def lesser_blocks(n, per, opening, neighbours, green, sigma):
    _, _, terms, orb, wide = green.shape

    def kernel(opening, neighbours, green, sigma, *outs):
        me = lax.axis_index("eloc")
        for k in range(n - 1, -1, -1):
            for i in range(per):
                atom = target_at(me, k, n) * per + i
                chosen = [sigma[0, atom]] + [sigma[0, neighbours[j, atom]] for j in range(terms - 1)]
                outs[k][i] = lesser_of([green[0, atom, j] for j in range(terms)], chosen)

    return pl.pallas_call(
        kernel,
        name="lesser",
        out_shape=[jax.ShapeDtypeStruct((per, orb, wide), BF16) for _ in range(n)],
        in_specs=[VMEM, SMEM, VMEM, VMEM],
        out_specs=[VMEM for _ in range(n)],
        compiler_params=limited(),
        cost_estimate=cost(400_000_000),
    )(opening, neighbours, green, sigma)


def prepared(occupancy, couplings):
    modes, per, orb, wide = couplings.shape

    def kernel(occupancy, couplings, right, left):
        for a in range(per):
            for m in range(modes):
                block = couplings[m, a]
                across = widened(block.astype(F32)).T
                occ = occupancy[m]
                right[a, m, :wide] = (across * (occ + 1.0)).astype(BF16)
                right[a, m, wide:] = (across * occ).astype(BF16)
            left[a, :orb] = jnp.concatenate([couplings[m, a][:, :orb] for m in range(modes)], 1)
            left[a, orb:] = jnp.concatenate([couplings[m, a][:, orb:] for m in range(modes)], 1)

    return pl.pallas_call(
        kernel,
        name="prepare",
        out_shape=[
            jax.ShapeDtypeStruct((per, modes, 2 * wide, wide), BF16),
            jax.ShapeDtypeStruct((per, 2 * orb, modes * orb), BF16),
        ],
        in_specs=[SMEM, VMEM],
        out_specs=[VMEM, VMEM],
        compiler_params=limited(),
        cost_estimate=cost(200_000_000),
    )(occupancy, couplings)


def mode_blocks(n, ks, shifts, extended, right, left):
    per, modes, _, wide = right.shape
    orb = wide // 2
    width = 2 if len(ks) % 2 == 0 else 1

    def kernel(shifts, extended, right, left, *rest):
        outs, stack = rest[: len(ks)], rest[-1]
        me = lax.axis_index("eloc")
        even = lax.axis_index("egrp") & 1 == 0
        places = {}
        for m in range(modes):
            for k in ks:
                e = target_at(me, k, n) + n
                above, below = place_of(me, e + shifts[m], n), place_of(me, e - shifts[m], n)
                above = jnp.where(even & (above >= 2 * n), above - 2 * n, above)
                below = jnp.where(even & (below < n), below + 2 * n, below)
                places[m, k] = (above, below)
        for a in range(per):
            for m in range(modes):
                rows = []
                for k in ks:
                    above, below = places[m, k]
                    rows.append(jnp.concatenate([extended[above, a], extended[below, a]], 1))
                stacked = jnp.concatenate(rows, 0)
                product = jnp.dot(stacked, right[a, m], preferred_element_type=F32).astype(BF16)
                for q in range(len(ks)):
                    p, w = divmod(q, width)
                    stack[a, p, m * orb : (m + 1) * orb, w * wide : (w + 1) * wide] = (
                        product[q * orb : (q + 1) * orb]
                    )
            for p in range(len(ks) // width):
                both = jnp.dot(left[a], stack[a, p], preferred_element_type=F32)
                for w in range(width):
                    piece = both[:, w * wide : (w + 1) * wide]
                    outs[p * width + w][a] = (piece[:orb] + turned(piece[orb:])).astype(BF16)

    return pl.pallas_call(
        kernel,
        out_shape=[jax.ShapeDtypeStruct((per, orb, wide), BF16) for _ in ks],
        in_specs=[SMEM, VMEM, VMEM, VMEM],
        out_specs=[VMEM for _ in ks],
        scratch_shapes=[pltpu.VMEM((per, len(ks) // width, modes * orb, width * wide), BF16)],
        compiler_params=limited(),
        cost_estimate=cost(400_000_000),
    )(shifts, extended, right, left)


def joined(n, blocks):
    per, orb, wide = blocks[0].shape

    def kernel(*refs):
        blocks, out, done = refs[:n], refs[n], refs[n + 1]
        me = lax.axis_index("eloc")
        copies = []
        for k in range(n):
            place = out.at[0, pl.ds(source_at(me, k, n) * per, per)]
            copies.append(pltpu.make_async_copy(blocks[k], place, done.at[k]))
        for copy in copies:
            copy.start()
        for copy in copies:
            copy.wait()

    return pl.pallas_call(
        kernel,
        name="join",
        out_shape=jax.ShapeDtypeStruct((1, n * per, orb, wide), BF16),
        in_specs=[VMEM for _ in blocks],
        out_specs=HBM,
        scratch_shapes=[pltpu.SemaphoreType.DMA((n,))],
        compiler_params=limited(),
    )(*blocks)


def swapped(n, k, block):
    return lax.ppermute(block, "eloc", [(i, partner(i, k, n)) for i in range(n)])


def traded(groups, first, block):
    pairs = []
    for i in range(first, groups - 1, 2):
        pairs += [(i, i + 1), (i + 1, i)]
    return lax.ppermute(block, "egrp", pairs)


def shards(green_blocks, sigma_prev, neighbours, couplings, occupancy, shifts):
    n, groups = lax.axis_size("eloc"), lax.axis_size("egrp")
    per = couplings.shape[1]
    made = lesser_blocks(n, per, opened(), neighbours.T, green_blocks, sigma_prev)
    held = [made[0]] + [swapped(n, k, made[k]) for k in range(1, n)]
    right, left = prepared(occupancy, couplings)
    here = jnp.stack(held)
    here, right, left = lax.optimization_barrier((here, right, left))
    outer = traded(groups, 1, here)
    inner = traded(groups, 0, here)
    extended = jnp.concatenate([inner, here, outer], 0)
    order = list(range(n - 1, -1, -1))
    made = mode_blocks(n, order, shifts, extended, right, left)[::-1]
    back = [made[0]] + [swapped(n, k, made[k]) for k in range(1, n)]
    return joined(n, back)


def solution(mesh):
    return jax.shard_map(
        shards,
        mesh=mesh,
        in_specs=(
            P(("egrp", "eloc"), None, None, None, None),
            P(("egrp", "eloc"), None, None, None),
            P(),
            P(None, "eloc", None, None),
            P(),
            P(),
        ),
        out_specs=P(("egrp", "eloc"), None, None, None),
        check_vma=False,
    )
```

```python
import jax
import jax.numpy as jnp
from jax import lax
from jax.experimental import pallas as pl
from jax.experimental.pallas import tpu as pltpu
from jax.sharding import PartitionSpec as P


VMEM = pl.BlockSpec(memory_space=pltpu.VMEM)
SMEM = pl.BlockSpec(memory_space=pltpu.SMEM)
HBM = pl.BlockSpec(memory_space=pltpu.HBM)
BF16 = jnp.bfloat16
F32 = jnp.float32
NT = (((1,), (1,)), ((), ()))


def limited():
    return pltpu.CompilerParams(vmem_limit_bytes=12 * 1024 * 1024)


def cost(flops):
    return pl.CostEstimate(flops=flops, bytes_accessed=1_000_000, transcendentals=0)


def two_power(n):
    return n & (n - 1) == 0


def partner(i, k, n):
    return i ^ k if two_power(n) else (i + k) % n


def target_at(me, k, n):
    return me ^ k if two_power(n) else lax.rem(me + k, n)


def source_at(me, k, n):
    return me ^ k if two_power(n) else lax.rem(me + n - k, n)


def place_of(me, t, n):
    if two_power(n):
        return (t & ~(n - 1)) + (me ^ (t & (n - 1)))
    inside = lax.rem(t, n)
    return t - inside + lax.rem(me - inside + n, n)


def turned(block):
    half = block.shape[-1] // 2
    return jnp.concatenate([-block[:, half:], block[:, :half]], -1)


def widened(block):
    return jnp.concatenate([block, turned(block)], 0)


def opened():
    def kernel(out):
        out[...] = jnp.zeros_like(out)

    return pl.pallas_call(
        kernel,
        name="opening",
        out_shape=jax.ShapeDtypeStruct((8, 128), jnp.int32),
        out_specs=VMEM,
        compiler_params=limited(),
        cost_estimate=cost(4_000_000_000),
    )()


def lesser_blocks(n, per, opening, neighbours, green, sigma):
    _, _, terms, orb, wide = green.shape

    def kernel(opening, neighbours, green, sigma, *rest):
        outs, (table, halves, done) = rest[:n], rest[n:]
        me = lax.axis_index("eloc")
        copy = pltpu.make_async_copy(neighbours, table, done)
        copy.start()
        spots = [(k, i, target_at(me, k, n) * per + i) for k in range(n - 1, -1, -1) for i in range(per)]

        def put_half(spot, j, other):
            k, i, atom = spot
            half = jnp.dot(green[0, atom, j], widened(sigma[0, other]), preferred_element_type=F32)
            half = half.astype(BF16)
            halves[k, i, j, :orb] = half
            halves[k, i, j, orb:] = turned(half)

        for spot in spots:
            put_half(spot, 0, spot[2])
        copy.wait()
        for spot in spots:
            for j in range(1, terms):
                put_half(spot, j, table[j - 1, spot[2]])
        for k, i, atom in spots:
            total = None
            for j in range(terms):
                term = lax.dot_general(halves[k, i, j], green[0, atom, j], NT, preferred_element_type=F32)
                total = term if total is None else total + term
            outs[k][i] = jnp.concatenate([total[:orb], -total[orb:]], 1).astype(BF16)

    return pl.pallas_call(
        kernel,
        name="lesser",
        out_shape=[jax.ShapeDtypeStruct((per, orb, wide), BF16) for _ in range(n)],
        in_specs=[VMEM, HBM, VMEM, VMEM],
        out_specs=[VMEM for _ in range(n)],
        scratch_shapes=[
            pltpu.SMEM(neighbours.shape, jnp.int32),
            pltpu.VMEM((n, per, terms, 2 * orb, wide), BF16),
            pltpu.SemaphoreType.DMA,
        ],
        compiler_params=limited(),
        cost_estimate=cost(400_000_000),
    )(opening, neighbours, green, sigma)


def prepared(occupancy, shifts, couplings):
    modes, per, orb, wide = couplings.shape

    def kernel(occupancy, shifts, couplings, right, left, moves):
        lane = lax.broadcasted_iota(jnp.int32, moves.shape, 1)
        row = jnp.zeros(moves.shape, jnp.int32)
        for m in range(modes):
            row = jnp.where(lane == m, shifts[m], row)
        moves[...] = row
        for a in range(per):
            for m in range(modes):
                block = couplings[m, a]
                across = widened(block.astype(F32)).T
                occ = occupancy[m]
                right[a, m, :wide] = (across * (occ + 1.0)).astype(BF16)
                right[a, m, wide:] = (across * occ).astype(BF16)
            left[a, :orb] = jnp.concatenate([couplings[m, a][:, :orb] for m in range(modes)], 1)
            left[a, orb:] = jnp.concatenate([couplings[m, a][:, orb:] for m in range(modes)], 1)

    return pl.pallas_call(
        kernel,
        name="prepare",
        out_shape=[
            jax.ShapeDtypeStruct((per, modes, 2 * wide, wide), BF16),
            jax.ShapeDtypeStruct((per, 2 * orb, modes * orb), BF16),
            jax.ShapeDtypeStruct((8, 128), jnp.int32),
        ],
        in_specs=[SMEM, SMEM, VMEM],
        out_specs=[VMEM, VMEM, VMEM],
        compiler_params=limited(),
        cost_estimate=cost(200_000_000),
    )(occupancy, shifts, couplings)


def mode_blocks(n, ks, moves, extended, right, left):
    per, modes, _, wide = right.shape
    orb = wide // 2
    width = 2 if len(ks) % 2 == 0 else 1

    def kernel(moves, extended, right, left, *rest):
        outs, stack = rest[: len(ks)], rest[-1]
        me = lax.axis_index("eloc")
        even = lax.axis_index("egrp") & 1 == 0
        row = moves[...]
        lane = lax.broadcasted_iota(jnp.int32, row.shape, 1)
        shifts = [jnp.max(jnp.where(lane == m, row, 0)) for m in range(modes)]
        places = {}
        for m in range(modes):
            for k in ks:
                e = target_at(me, k, n) + n
                above, below = place_of(me, e + shifts[m], n), place_of(me, e - shifts[m], n)
                above = jnp.where(even & (above >= 2 * n), above - 2 * n, above)
                below = jnp.where(even & (below < n), below + 2 * n, below)
                places[m, k] = (above, below)
        for a in range(per):
            for m in range(modes):
                rows = []
                for k in ks:
                    above, below = places[m, k]
                    rows.append(jnp.concatenate([extended[above, a], extended[below, a]], 1))
                stacked = jnp.concatenate(rows, 0)
                product = jnp.dot(stacked, right[a, m], preferred_element_type=F32).astype(BF16)
                for q in range(len(ks)):
                    p, w = divmod(q, width)
                    stack[a, p, m * orb : (m + 1) * orb, w * wide : (w + 1) * wide] = (
                        product[q * orb : (q + 1) * orb]
                    )
            for p in range(len(ks) // width):
                both = jnp.dot(left[a], stack[a, p], preferred_element_type=F32)
                for w in range(width):
                    piece = both[:, w * wide : (w + 1) * wide]
                    outs[p * width + w][a] = (piece[:orb] + turned(piece[orb:])).astype(BF16)

    return pl.pallas_call(
        kernel,
        out_shape=[jax.ShapeDtypeStruct((per, orb, wide), BF16) for _ in ks],
        in_specs=[VMEM, VMEM, VMEM, VMEM],
        out_specs=[VMEM for _ in ks],
        scratch_shapes=[pltpu.VMEM((per, len(ks) // width, modes * orb, width * wide), BF16)],
        compiler_params=limited(),
        cost_estimate=cost(400_000_000),
    )(moves, extended, right, left)


def joined(n, blocks):
    per, orb, wide = blocks[0].shape

    def kernel(*refs):
        blocks, out, done = refs[:n], refs[n], refs[n + 1]
        me = lax.axis_index("eloc")
        copies = []
        for k in range(n):
            place = out.at[0, pl.ds(source_at(me, k, n) * per, per)]
            copies.append(pltpu.make_async_copy(blocks[k], place, done.at[k]))
        for copy in copies:
            copy.start()
        for copy in copies:
            copy.wait()

    return pl.pallas_call(
        kernel,
        name="join",
        out_shape=jax.ShapeDtypeStruct((1, n * per, orb, wide), BF16),
        in_specs=[VMEM for _ in blocks],
        out_specs=HBM,
        scratch_shapes=[pltpu.SemaphoreType.DMA((n,))],
        compiler_params=limited(),
    )(*blocks)


def swapped(n, k, block):
    return lax.ppermute(block, "eloc", [(i, partner(i, k, n)) for i in range(n)])


def traded(groups, first, block):
    pairs = []
    for i in range(first, groups - 1, 2):
        pairs += [(i, i + 1), (i + 1, i)]
    return lax.ppermute(block, "egrp", pairs)


def shards(green_blocks, sigma_prev, neighbours, couplings, occupancy, shifts):
    n, groups = lax.axis_size("eloc"), lax.axis_size("egrp")
    per = couplings.shape[1]
    made = lesser_blocks(n, per, opened(), neighbours.T, green_blocks, sigma_prev)
    held = [made[0]] + [swapped(n, k, made[k]) for k in range(1, n)]
    right, left, moves = prepared(occupancy, shifts, couplings)
    soon = jnp.stack(held[: n // 2])
    early = traded(groups, 1, soon)
    here = jnp.stack(held)
    here, right, left, moves = lax.optimization_barrier((here, right, left, moves))
    outer = traded(groups, 1, here[n // 2 :])
    inner = traded(groups, 0, here)
    extended = jnp.concatenate([inner, here, early, outer], 0)
    order = list(range(n - 1, -1, -1))
    made = mode_blocks(n, order, moves, extended, right, left)[::-1]
    back = [made[0]] + [swapped(n, k, made[k]) for k in range(1, n)]
    return joined(n, back)


def solution(mesh):
    return jax.shard_map(
        shards,
        mesh=mesh,
        in_specs=(
            P(("egrp", "eloc"), None, None, None, None),
            P(("egrp", "eloc"), None, None, None),
            P(),
            P(None, "eloc", None, None),
            P(),
            P(),
        ),
        out_specs=P(("egrp", "eloc"), None, None, None),
        check_vma=False,
    )
```

```python
import jax
import jax.numpy as jnp
from jax import lax
from jax.experimental import pallas as pl
from jax.experimental.pallas import tpu as pltpu
from jax.sharding import PartitionSpec as P


VMEM = pl.BlockSpec(memory_space=pltpu.VMEM)
SMEM = pl.BlockSpec(memory_space=pltpu.SMEM)
HBM = pl.BlockSpec(memory_space=pltpu.HBM)
BF16 = jnp.bfloat16
F32 = jnp.float32
NT = (((1,), (1,)), ((), ()))


def limited():
    return pltpu.CompilerParams(vmem_limit_bytes=12 * 1024 * 1024)


def cost(flops):
    return pl.CostEstimate(flops=flops, bytes_accessed=1_000_000, transcendentals=0)


def two_power(n):
    return n & (n - 1) == 0


def partner(i, k, n):
    return i ^ k if two_power(n) else (i + k) % n


def target_at(me, k, n):
    return me ^ k if two_power(n) else lax.rem(me + k, n)


def source_at(me, k, n):
    return me ^ k if two_power(n) else lax.rem(me + n - k, n)


def place_of(me, t, n):
    if two_power(n):
        return (t & ~(n - 1)) + (me ^ (t & (n - 1)))
    inside = lax.rem(t, n)
    return t - inside + lax.rem(me - inside + n, n)


def turned(block):
    half = block.shape[-1] // 2
    return jnp.concatenate([-block[:, half:], block[:, :half]], -1)


def widened(block):
    return jnp.concatenate([block, turned(block)], 0)


def opened():
    def kernel(out):
        out[...] = jnp.zeros_like(out)

    return pl.pallas_call(
        kernel,
        name="opening",
        out_shape=jax.ShapeDtypeStruct((8, 128), jnp.int32),
        out_specs=VMEM,
        compiler_params=limited(),
        cost_estimate=cost(4_000_000_000),
    )()


def lesser_blocks(n, per, opening, neighbours, green, sigma):
    _, _, terms, orb, wide = green.shape

    def kernel(opening, neighbours, green, sigma, *rest):
        outs, (table, halves, done) = rest[:n], rest[n:]
        me = lax.axis_index("eloc")
        copy = pltpu.make_async_copy(neighbours, table, done)
        copy.start()
        spots = [(k, i, target_at(me, k, n) * per + i) for k in range(n - 1, -1, -1) for i in range(per)]

        def put_half(spot, j, other):
            k, i, atom = spot
            half = jnp.dot(green[0, atom, j], widened(sigma[0, other]), preferred_element_type=F32)
            half = half.astype(BF16)
            halves[k, i, j, :orb] = half
            halves[k, i, j, orb:] = turned(half)

        for spot in spots:
            put_half(spot, 0, spot[2])
        copy.wait()
        for spot in spots:
            for j in range(1, terms):
                put_half(spot, j, table[j - 1, spot[2]])
        for k, i, atom in spots:
            total = None
            for j in range(terms):
                term = lax.dot_general(halves[k, i, j], green[0, atom, j], NT, preferred_element_type=F32)
                total = term if total is None else total + term
            outs[k][i] = jnp.concatenate([total[:orb], -total[orb:]], 1).astype(BF16)

    return pl.pallas_call(
        kernel,
        name="lesser",
        out_shape=[jax.ShapeDtypeStruct((per, orb, wide), BF16) for _ in range(n)],
        in_specs=[VMEM, HBM, VMEM, VMEM],
        out_specs=[VMEM for _ in range(n)],
        scratch_shapes=[
            pltpu.SMEM(neighbours.shape, jnp.int32),
            pltpu.VMEM((n, per, terms, 2 * orb, wide), BF16),
            pltpu.SemaphoreType.DMA,
        ],
        compiler_params=limited(),
        cost_estimate=cost(400_000_000),
    )(opening, neighbours, green, sigma)


def prepared(occupancy, shifts, couplings):
    modes, per, orb, wide = couplings.shape

    def kernel(occupancy, shifts, couplings, right, left, moves):
        lane = lax.broadcasted_iota(jnp.int32, moves.shape, 1)
        row = jnp.zeros(moves.shape, jnp.int32)
        for m in range(modes):
            row = jnp.where(lane == m, shifts[m], row)
        moves[...] = row
        for a in range(per):
            for m in range(modes):
                block = couplings[m, a]
                across = widened(block.astype(F32)).T
                occ = occupancy[m]
                right[a, m, :wide] = (across * (occ + 1.0)).astype(BF16)
                right[a, m, wide:] = (across * occ).astype(BF16)
            left[a, :orb] = jnp.concatenate([couplings[m, a][:, :orb] for m in range(modes)], 1)
            left[a, orb:] = jnp.concatenate([couplings[m, a][:, orb:] for m in range(modes)], 1)

    return pl.pallas_call(
        kernel,
        name="prepare",
        out_shape=[
            jax.ShapeDtypeStruct((per, modes, 2 * wide, wide), BF16),
            jax.ShapeDtypeStruct((per, 2 * orb, modes * orb), BF16),
            jax.ShapeDtypeStruct((8, 128), jnp.int32),
        ],
        in_specs=[SMEM, SMEM, VMEM],
        out_specs=[VMEM, VMEM, VMEM],
        compiler_params=limited(),
        cost_estimate=cost(200_000_000),
    )(occupancy, shifts, couplings)


def read_moves(moves, modes):
    row = moves[...]
    lane = lax.broadcasted_iota(jnp.int32, row.shape, 1)
    return [jnp.max(jnp.where(lane == m, row, 0)) for m in range(modes)]


def put_products(stack, a, m, product, count, width):
    orb, wide = product.shape[0] // count, product.shape[1]
    for q in range(count):
        p, w = divmod(q, width)
        stack[a, p, m * orb : (m + 1) * orb, w * wide : (w + 1) * wide] = product[q * orb : (q + 1) * orb]


def outer_products(stack, left, a, count, width):
    orb = left.shape[1] // 2
    pieces = []
    for p in range(count // width):
        both = jnp.dot(left[a], stack[a, p], preferred_element_type=F32)
        for w in range(width):
            piece = both[:, w * 2 * orb : (w + 1) * 2 * orb]
            pieces.append(piece[:orb] + turned(piece[orb:]))
    return pieces


def first_modes(n, moves, extended, right, left):
    per, modes, _, wide = right.shape
    orb = wide // 2
    width = 2 if n % 2 == 0 else 1

    def kernel(moves, extended, right, left, *rest):
        outs, stack = rest[:n], rest[-1]
        me = lax.axis_index("eloc")
        even = lax.axis_index("egrp") & 1 == 0
        shifts = read_moves(moves, modes)
        places = {}
        for m in range(modes):
            for k in range(n):
                e = target_at(me, k, n) + n
                above, below = place_of(me, e + shifts[m], n), place_of(me, e - shifts[m], n)
                above = jnp.where(even & (above >= 2 * n), above - 2 * n, above)
                below = jnp.where(even & (below < n), below + 2 * n, below)
                places[m, k] = (above, below)
        for a in range(per):
            for m in range(modes):
                rows = [
                    jnp.concatenate([extended[places[m, k][0], a], extended[places[m, k][1], a]], 1)
                    for k in range(n)
                ]
                product = jnp.dot(jnp.concatenate(rows, 0), right[a, m], preferred_element_type=F32)
                put_products(stack, a, m, product.astype(BF16), n, width)
            for k, piece in enumerate(outer_products(stack, left, a, n, width)):
                outs[k][a] = piece

    return pl.pallas_call(
        kernel,
        name="first_modes",
        out_shape=[jax.ShapeDtypeStruct((per, orb, wide), F32) for _ in range(n)],
        in_specs=[VMEM for _ in range(4)],
        out_specs=[VMEM for _ in range(n)],
        scratch_shapes=[pltpu.VMEM((per, n // width, modes * orb, width * wide), BF16)],
        compiler_params=limited(),
        cost_estimate=cost(400_000_000),
    )(moves, extended, right, left)


def last_modes(n, groups, ks, moves, outer, partials, right, left):
    per, modes, _, wide = right.shape
    orb, count, late = wide // 2, len(ks), n - outer.shape[0]
    width = 2 if count % 2 == 0 else 1

    def kernel(moves, outer, right, left, *rest):
        partials, outs, stack = rest[:count], rest[count : 2 * count], rest[-1]
        me = lax.axis_index("eloc")
        even = lax.axis_index("egrp") & 1 == 0
        group = lax.axis_index("egrp")
        within = (group > 0) & (group < groups - 1)
        begin = pl.multiple_of(jnp.where(even, wide, 0), wide)
        shifts = read_moves(moves, modes)
        places = {}
        for m in range(modes):
            for k in ks:
                e = target_at(me, k, n) + n
                t = jnp.where(even, e - shifts[m], e + shifts[m])
                outside = jnp.where(even, t < n, t >= 2 * n) & within
                base = jnp.where(even, 0, 2 * n)
                slot = jnp.where(outside, place_of(me, t, n) - base, 0)
                places[m, k] = (slot >= late, jnp.maximum(slot - late, 0))
        for a in range(per):
            for m in range(modes):
                rows = []
                for k in ks:
                    held, slot = places[m, k]
                    block = outer[slot, a]
                    rows.append(jnp.where(held, block, jnp.zeros_like(block)))
                weights = right[a, m, pl.ds(begin, wide)]
                product = jnp.dot(jnp.concatenate(rows, 0), weights, preferred_element_type=F32)
                put_products(stack, a, m, product.astype(BF16), count, width)
            for q, piece in enumerate(outer_products(stack, left, a, count, width)):
                outs[q][a] = (partials[q][a] + piece).astype(BF16)

    return pl.pallas_call(
        kernel,
        out_shape=[jax.ShapeDtypeStruct((per, orb, wide), BF16) for _ in ks],
        in_specs=[VMEM for _ in range(4 + count)],
        out_specs=[VMEM for _ in ks],
        scratch_shapes=[pltpu.VMEM((per, count // width, modes * orb, width * wide), BF16)],
        compiler_params=limited(),
        cost_estimate=cost(400_000_000),
    )(moves, outer, right, left, *[partials[k] for k in ks])


def joined(n, blocks):
    per, orb, wide = blocks[0].shape

    def kernel(*refs):
        blocks, out, done = refs[:n], refs[n], refs[n + 1]
        me = lax.axis_index("eloc")
        copies = []
        for k in range(n):
            place = out.at[0, pl.ds(source_at(me, k, n) * per, per)]
            copies.append(pltpu.make_async_copy(blocks[k], place, done.at[k]))
        for copy in copies:
            copy.start()
        for copy in copies:
            copy.wait()

    return pl.pallas_call(
        kernel,
        name="join",
        out_shape=jax.ShapeDtypeStruct((1, n * per, orb, wide), BF16),
        in_specs=[VMEM for _ in blocks],
        out_specs=HBM,
        scratch_shapes=[pltpu.SemaphoreType.DMA((n,))],
        compiler_params=limited(),
    )(*blocks)


def swapped(n, k, block):
    return lax.ppermute(block, "eloc", [(i, partner(i, k, n)) for i in range(n)])


def traded(groups, first, block):
    pairs = []
    for i in range(first, groups - 1 + (groups % 2 == 0) * first, 2):
        pairs += [(i, (i + 1) % groups), ((i + 1) % groups, i)]
    return lax.ppermute(block, "egrp", pairs)


def inside(groups, block):
    me = lax.axis_index("egrp")
    edge = (me == 0) | (me == groups - 1)
    return jnp.where(edge, jnp.zeros_like(block), block)


def shards(green_blocks, sigma_prev, neighbours, couplings, occupancy, shifts):
    n, groups = lax.axis_size("eloc"), lax.axis_size("egrp")
    per = couplings.shape[1]
    made = lesser_blocks(n, per, opened(), neighbours.T, green_blocks, sigma_prev)
    held = [made[0]] + [swapped(n, k, made[k]) for k in range(1, n)]
    right, left, moves = prepared(occupancy, shifts, couplings)
    soon = jnp.stack(held[: n // 2])
    early = traded(groups, 1, soon)
    here = jnp.stack(held)
    here, right, left, moves = lax.optimization_barrier((here, right, left, moves))
    outer = traded(groups, 1, here[n // 2 :])
    inner = traded(groups, 0, here)
    missing = jnp.zeros_like(outer)
    partials = first_modes(n, moves, jnp.concatenate([inner, here, inside(groups, early), missing], 0), right, left)
    back = {}
    for ks in (list(range(n)),):
        made = last_modes(n, groups, ks, moves, outer, partials, right, left)
        for k, block in zip(ks, made):
            back[k] = swapped(n, k, block) if k else block
    back = [back[k] for k in range(n)]
    return joined(n, back)


def solution(mesh):
    return jax.shard_map(
        shards,
        mesh=mesh,
        in_specs=(
            P(("egrp", "eloc"), None, None, None, None),
            P(("egrp", "eloc"), None, None, None),
            P(),
            P(None, "eloc", None, None),
            P(),
            P(),
        ),
        out_specs=P(("egrp", "eloc"), None, None, None),
        check_vma=False,
    )
```

```python
import jax
import jax.numpy as jnp
from jax import lax
from jax.experimental import pallas as pl
from jax.experimental.pallas import tpu as pltpu
from jax.sharding import PartitionSpec as P


VMEM = pl.BlockSpec(memory_space=pltpu.VMEM)
SMEM = pl.BlockSpec(memory_space=pltpu.SMEM)
HBM = pl.BlockSpec(memory_space=pltpu.HBM)
BF16 = jnp.bfloat16
F32 = jnp.float32
NT = (((1,), (1,)), ((), ()))


def limited():
    return pltpu.CompilerParams(vmem_limit_bytes=12 * 1024 * 1024)


def cost(flops):
    return pl.CostEstimate(flops=flops, bytes_accessed=1_000_000, transcendentals=0)


def two_power(n):
    return n & (n - 1) == 0


def partner(i, k, n):
    return i ^ k if two_power(n) else (i + k) % n


def target_at(me, k, n):
    return me ^ k if two_power(n) else lax.rem(me + k, n)


def source_at(me, k, n):
    return me ^ k if two_power(n) else lax.rem(me + n - k, n)


def place_of(me, t, n):
    if two_power(n):
        return (t & ~(n - 1)) + (me ^ (t & (n - 1)))
    inside = lax.rem(t, n)
    return t - inside + lax.rem(me - inside + n, n)


def turned(block):
    half = block.shape[-1] // 2
    return jnp.concatenate([-block[:, half:], block[:, :half]], -1)


def widened(block):
    return jnp.concatenate([block, turned(block)], 0)


def opened():
    def kernel(out):
        out[...] = jnp.zeros_like(out)

    return pl.pallas_call(
        kernel,
        name="opening",
        out_shape=jax.ShapeDtypeStruct((8, 128), jnp.int32),
        out_specs=VMEM,
        compiler_params=limited(),
        cost_estimate=cost(4_000_000_000),
    )()


def lesser_blocks(n, per, opening, neighbours, green, sigma):
    _, _, terms, orb, wide = green.shape

    def kernel(opening, neighbours, green, sigma, *rest):
        outs, (table, halves, done) = rest[:n], rest[n:]
        me = lax.axis_index("eloc")
        copy = pltpu.make_async_copy(neighbours, table, done)
        copy.start()
        spots = [(k, i, target_at(me, k, n) * per + i) for k in range(n) for i in range(per)]

        def put_half(spot, j, other):
            k, i, atom = spot
            half = jnp.dot(green[0, atom, j], widened(sigma[0, other]), preferred_element_type=F32)
            half = half.astype(BF16)
            halves[k, i, j, :orb] = half
            halves[k, i, j, orb:] = turned(half)

        for spot in spots:
            put_half(spot, 0, spot[2])
        copy.wait()
        for spot in spots:
            for j in range(1, terms):
                put_half(spot, j, table[j - 1, spot[2]])
        for k, i, atom in spots:
            total = None
            for j in range(terms):
                term = lax.dot_general(halves[k, i, j], green[0, atom, j], NT, preferred_element_type=F32)
                total = term if total is None else total + term
            outs[k][i] = jnp.concatenate([total[:orb], -total[orb:]], 1).astype(BF16)

    return pl.pallas_call(
        kernel,
        name="lesser",
        out_shape=[jax.ShapeDtypeStruct((per, orb, wide), BF16) for _ in range(n)],
        in_specs=[VMEM, HBM, VMEM, VMEM],
        out_specs=[VMEM for _ in range(n)],
        scratch_shapes=[
            pltpu.SMEM(neighbours.shape, jnp.int32),
            pltpu.VMEM((n, per, terms, 2 * orb, wide), BF16),
            pltpu.SemaphoreType.DMA,
        ],
        compiler_params=limited(),
        cost_estimate=cost(400_000_000),
    )(opening, neighbours, green, sigma)


def prepared(occupancy, shifts, couplings):
    modes, per, orb, wide = couplings.shape

    def kernel(occupancy, shifts, couplings, right, left, moves):
        lane = lax.broadcasted_iota(jnp.int32, moves.shape, 1)
        row = jnp.zeros(moves.shape, jnp.int32)
        for m in range(modes):
            row = jnp.where(lane == m, shifts[m], row)
        moves[...] = row
        for a in range(per):
            for m in range(modes):
                block = couplings[m, a]
                across = widened(block.astype(F32)).T
                occ = occupancy[m]
                right[a, m, :wide] = (across * (occ + 1.0)).astype(BF16)
                right[a, m, wide:] = (across * occ).astype(BF16)
            left[a, :orb] = jnp.concatenate([couplings[m, a][:, :orb] for m in range(modes)], 1)
            left[a, orb:] = jnp.concatenate([couplings[m, a][:, orb:] for m in range(modes)], 1)

    return pl.pallas_call(
        kernel,
        name="prepare",
        out_shape=[
            jax.ShapeDtypeStruct((per, modes, 2 * wide, wide), BF16),
            jax.ShapeDtypeStruct((per, 2 * orb, modes * orb), BF16),
            jax.ShapeDtypeStruct((8, 128), jnp.int32),
        ],
        in_specs=[SMEM, SMEM, VMEM],
        out_specs=[VMEM, VMEM, VMEM],
        compiler_params=limited(),
        cost_estimate=cost(200_000_000),
    )(occupancy, shifts, couplings)


def read_moves(moves, modes):
    row = moves[...]
    lane = lax.broadcasted_iota(jnp.int32, row.shape, 1)
    return [jnp.max(jnp.where(lane == m, row, 0)) for m in range(modes)]


def put_products(stack, a, m, product, count, width):
    orb, wide = product.shape[0] // count, product.shape[1]
    for q in range(count):
        p, w = divmod(q, width)
        stack[a, p, m * orb : (m + 1) * orb, w * wide : (w + 1) * wide] = product[q * orb : (q + 1) * orb]


def outer_products(stack, left, a, count, width):
    orb = left.shape[1] // 2
    pieces = []
    for p in range(count // width):
        both = jnp.dot(left[a], stack[a, p], preferred_element_type=F32)
        for w in range(width):
            piece = both[:, w * 2 * orb : (w + 1) * 2 * orb]
            pieces.append(piece[:orb] + turned(piece[orb:]))
    return pieces


def first_modes(n, moves, extended, right, left):
    per, modes, _, wide = right.shape
    orb = wide // 2
    width = 2 if n % 2 == 0 else 1

    def kernel(moves, extended, right, left, *rest):
        outs, stack = rest[:n], rest[-1]
        me = lax.axis_index("eloc")
        even = lax.axis_index("egrp") & 1 == 0
        shifts = read_moves(moves, modes)
        places = {}
        for m in range(modes):
            for k in range(n):
                e = target_at(me, k, n) + n
                above, below = place_of(me, e + shifts[m], n), place_of(me, e - shifts[m], n)
                above = jnp.where(even & (above >= 2 * n), above - 2 * n, above)
                below = jnp.where(even & (below < n), below + 2 * n, below)
                places[m, k] = (above, below)
        for a in range(per):
            for m in range(modes):
                rows = [
                    jnp.concatenate([extended[places[m, k][0], a], extended[places[m, k][1], a]], 1)
                    for k in range(n)
                ]
                product = jnp.dot(jnp.concatenate(rows, 0), right[a, m], preferred_element_type=F32)
                put_products(stack, a, m, product.astype(BF16), n, width)
        for a in range(per):
            for k, piece in enumerate(outer_products(stack, left, a, n, width)):
                outs[k][a] = piece

    return pl.pallas_call(
        kernel,
        name="first_modes",
        out_shape=[jax.ShapeDtypeStruct((per, orb, wide), F32) for _ in range(n)],
        in_specs=[VMEM for _ in range(4)],
        out_specs=[VMEM for _ in range(n)],
        scratch_shapes=[pltpu.VMEM((per, n // width, modes * orb, width * wide), BF16)],
        compiler_params=limited(),
        cost_estimate=cost(400_000_000),
    )(moves, extended, right, left)


def last_modes(n, groups, ks, moves, outer, partials, right, left):
    per, modes, _, wide = right.shape
    orb, count, late = wide // 2, len(ks), n - outer.shape[0]
    width = 2 if count % 2 == 0 else 1

    def kernel(moves, outer, right, left, *rest):
        partials, outs, (made, stack) = rest[:count], rest[count : 2 * count], rest[2 * count :]
        me = lax.axis_index("eloc")
        even = lax.axis_index("egrp") & 1 == 0
        group = lax.axis_index("egrp")
        within = (group > 0) & (group < groups - 1)
        begin = pl.multiple_of(jnp.where(even, wide, 0), wide)
        shifts = read_moves(moves, modes)
        places = {}
        for m in range(modes):
            for k in ks:
                e = target_at(me, k, n) + n
                t = jnp.where(even, e - shifts[m], e + shifts[m])
                outside = jnp.where(even, t < n, t >= 2 * n) & within
                base = jnp.where(even, 0, 2 * n)
                slot = jnp.where(outside, place_of(me, t, n) - base, 0)
                places[m, k] = (slot >= late, jnp.maximum(slot - late, 0))
        for a in range(per):
            blocks = jnp.concatenate([outer[b, a] for b in range(n - late)], 0)
            for m in range(0, modes, 2):
                both = [right[a, m + i, pl.ds(begin, wide)] for i in range(min(2, modes - m))]
                product = jnp.dot(blocks, jnp.concatenate(both, 1), preferred_element_type=F32).astype(BF16)
                for i in range(len(both)):
                    for b in range(n - late):
                        made[a, b, m + i] = product[b * orb : (b + 1) * orb, i * wide : (i + 1) * wide]
        for a in range(per):
            for m in range(modes):
                for q, k in enumerate(ks):
                    held, slot = places[m, k]
                    block = made[a, slot, m]
                    p, w = divmod(q, width)
                    stack[a, p, m * orb : (m + 1) * orb, w * wide : (w + 1) * wide] = jnp.where(
                        held, block, jnp.zeros_like(block)
                    )
        for a in range(per):
            for q, piece in enumerate(outer_products(stack, left, a, count, width)):
                outs[q][a] = (partials[q][a] + piece).astype(BF16)

    return pl.pallas_call(
        kernel,
        out_shape=[jax.ShapeDtypeStruct((per, orb, wide), BF16) for _ in ks],
        in_specs=[VMEM for _ in range(4 + count)],
        out_specs=[VMEM for _ in ks],
        scratch_shapes=[
            pltpu.VMEM((per, n - late, modes, orb, wide), BF16),
            pltpu.VMEM((per, count // width, modes * orb, width * wide), BF16),
        ],
        compiler_params=limited(),
        cost_estimate=cost(400_000_000),
    )(moves, outer, right, left, *[partials[k] for k in ks])


def joined(n, blocks):
    per, orb, wide = blocks[0].shape

    def kernel(*refs):
        blocks, out, done = refs[:n], refs[n], refs[n + 1]
        me = lax.axis_index("eloc")
        copies = []
        for k in range(n):
            place = out.at[0, pl.ds(source_at(me, k, n) * per, per)]
            copies.append(pltpu.make_async_copy(blocks[k], place, done.at[k]))
        for copy in copies:
            copy.start()
        for copy in copies:
            copy.wait()

    return pl.pallas_call(
        kernel,
        name="join",
        out_shape=jax.ShapeDtypeStruct((1, n * per, orb, wide), BF16),
        in_specs=[VMEM for _ in blocks],
        out_specs=HBM,
        scratch_shapes=[pltpu.SemaphoreType.DMA((n,))],
        compiler_params=limited(),
    )(*blocks)


def swapped(n, k, block):
    return lax.ppermute(block, "eloc", [(i, partner(i, k, n)) for i in range(n)])


def traded(groups, first, block):
    pairs = []
    for i in range(first, groups - 1 + (groups % 2 == 0) * first, 2):
        pairs += [(i, (i + 1) % groups), ((i + 1) % groups, i)]
    return lax.ppermute(block, "egrp", pairs)


def inside(groups, block):
    me = lax.axis_index("egrp")
    edge = (me == 0) | (me == groups - 1)
    return jnp.where(edge, jnp.zeros_like(block), block)


def shards(green_blocks, sigma_prev, neighbours, couplings, occupancy, shifts):
    n, groups = lax.axis_size("eloc"), lax.axis_size("egrp")
    per = couplings.shape[1]
    made = lesser_blocks(n, per, opened(), neighbours.T, green_blocks, sigma_prev)
    held = [made[0]] + [swapped(n, k, made[k]) for k in range(1, n)]
    right, left, moves = prepared(occupancy, shifts, couplings)
    soon = jnp.stack(held[: n // 2])
    early = traded(groups, 1, soon)
    here = jnp.stack(held)
    here, right, left, moves = lax.optimization_barrier((here, right, left, moves))
    outer = traded(groups, 1, here[n // 2 :])
    inner = traded(groups, 0, here)
    missing = jnp.zeros_like(outer)
    partials = first_modes(n, moves, jnp.concatenate([inner, here, inside(groups, early), missing], 0), right, left)
    back = {}
    for ks in (list(range(n)),):
        made = last_modes(n, groups, ks, moves, outer, partials, right, left)
        for k, block in zip(ks, made):
            back[k] = swapped(n, k, block) if k else block
    back = [back[k] for k in range(n)]
    return joined(n, back)


def solution(mesh):
    return jax.shard_map(
        shards,
        mesh=mesh,
        in_specs=(
            P(("egrp", "eloc"), None, None, None, None),
            P(("egrp", "eloc"), None, None, None),
            P(),
            P(None, "eloc", None, None),
            P(),
            P(),
        ),
        out_specs=P(("egrp", "eloc"), None, None, None),
        check_vma=False,
    )
```

```python
import jax
import jax.numpy as jnp
from jax import lax
from jax.experimental import pallas as pl
from jax.experimental.pallas import tpu as pltpu
from jax.sharding import PartitionSpec as P


VMEM = pl.BlockSpec(memory_space=pltpu.VMEM)
SMEM = pl.BlockSpec(memory_space=pltpu.SMEM)
HBM = pl.BlockSpec(memory_space=pltpu.HBM)
BF16 = jnp.bfloat16
F32 = jnp.float32
NT = (((1,), (1,)), ((), ()))


def limited():
    return pltpu.CompilerParams(vmem_limit_bytes=12 * 1024 * 1024)


def cost(flops):
    return pl.CostEstimate(flops=flops, bytes_accessed=1_000_000, transcendentals=0)


def two_power(n):
    return n & (n - 1) == 0


def partner(i, k, n):
    return i ^ k if two_power(n) else (i + k) % n


def target_at(me, k, n):
    return me ^ k if two_power(n) else lax.rem(me + k, n)


def source_at(me, k, n):
    return me ^ k if two_power(n) else lax.rem(me + n - k, n)


def place_of(me, t, n):
    if two_power(n):
        return (t & ~(n - 1)) + (me ^ (t & (n - 1)))
    inside = lax.rem(t, n)
    return t - inside + lax.rem(me - inside + n, n)


def turned(block):
    half = block.shape[-1] // 2
    return jnp.concatenate([-block[:, half:], block[:, :half]], -1)


def widened(block):
    return jnp.concatenate([block, turned(block)], 0)


def opened():
    def kernel(out):
        out[...] = jnp.zeros_like(out)

    return pl.pallas_call(
        kernel,
        name="opening",
        out_shape=jax.ShapeDtypeStruct((8, 128), jnp.int32),
        out_specs=VMEM,
        compiler_params=limited(),
        cost_estimate=cost(4_000_000_000),
    )()


def lesser_blocks(n, per, opening, neighbours, green, sigma):
    _, _, terms, orb, wide = green.shape

    def kernel(opening, neighbours, green, sigma, *rest):
        outs, (table, halves, done) = rest[:n], rest[n:]
        me = lax.axis_index("eloc")
        copy = pltpu.make_async_copy(neighbours, table, done)
        copy.start()
        spots = [(k, i, target_at(me, k, n) * per + i) for k in range(n - 1, -1, -1) for i in range(per)]

        def put_half(spot, j, other):
            k, i, atom = spot
            half = jnp.dot(green[0, atom, j], widened(sigma[0, other]), preferred_element_type=F32)
            half = half.astype(BF16)
            halves[k, i, j, :orb] = half
            halves[k, i, j, orb:] = turned(half)

        for spot in spots:
            put_half(spot, 0, spot[2])
        copy.wait()
        for spot in spots:
            for j in range(1, terms):
                put_half(spot, j, table[j - 1, spot[2]])
        for k, i, atom in spots:
            total = None
            for j in range(terms):
                term = lax.dot_general(halves[k, i, j], green[0, atom, j], NT, preferred_element_type=F32)
                total = term if total is None else total + term
            outs[k][i] = jnp.concatenate([total[:orb], -total[orb:]], 1).astype(BF16)

    return pl.pallas_call(
        kernel,
        name="lesser",
        out_shape=[jax.ShapeDtypeStruct((per, orb, wide), BF16) for _ in range(n)],
        in_specs=[VMEM, HBM, VMEM, VMEM],
        out_specs=[VMEM for _ in range(n)],
        scratch_shapes=[
            pltpu.SMEM(neighbours.shape, jnp.int32),
            pltpu.VMEM((n, per, terms, 2 * orb, wide), BF16),
            pltpu.SemaphoreType.DMA,
        ],
        compiler_params=limited(),
        cost_estimate=cost(400_000_000),
    )(opening, neighbours, green, sigma)


def prepared(occupancy, shifts, couplings):
    modes, per, orb, wide = couplings.shape

    def kernel(occupancy, shifts, couplings, right, left, moves):
        lane = lax.broadcasted_iota(jnp.int32, moves.shape, 1)
        row = jnp.zeros(moves.shape, jnp.int32)
        for m in range(modes):
            row = jnp.where(lane == m, shifts[m], row)
        moves[...] = row
        for a in range(per):
            for m in range(modes):
                block = couplings[m, a]
                across = widened(block.astype(F32)).T
                occ = occupancy[m]
                right[a, m, :wide] = (across * (occ + 1.0)).astype(BF16)
                right[a, m, wide:] = (across * occ).astype(BF16)
            left[a, :orb] = jnp.concatenate([couplings[m, a][:, :orb] for m in range(modes)], 1)
            left[a, orb:] = jnp.concatenate([couplings[m, a][:, orb:] for m in range(modes)], 1)

    return pl.pallas_call(
        kernel,
        name="prepare",
        out_shape=[
            jax.ShapeDtypeStruct((per, modes, 2 * wide, wide), BF16),
            jax.ShapeDtypeStruct((per, 2 * orb, modes * orb), BF16),
            jax.ShapeDtypeStruct((8, 128), jnp.int32),
        ],
        in_specs=[SMEM, SMEM, VMEM],
        out_specs=[VMEM, VMEM, VMEM],
        compiler_params=limited(),
        cost_estimate=cost(200_000_000),
    )(occupancy, shifts, couplings)


def read_moves(moves, modes):
    row = moves[...]
    lane = lax.broadcasted_iota(jnp.int32, row.shape, 1)
    return [jnp.max(jnp.where(lane == m, row, 0)) for m in range(modes)]


def put_products(stack, a, m, product, count, width):
    orb, wide = product.shape[0] // count, product.shape[1]
    for q in range(count):
        p, w = divmod(q, width)
        stack[a, p, m * orb : (m + 1) * orb, w * wide : (w + 1) * wide] = product[q * orb : (q + 1) * orb]


def outer_products(stack, left, a, count, width):
    orb = left.shape[1] // 2
    pieces = []
    for p in range(count // width):
        both = jnp.dot(left[a], stack[a, p], preferred_element_type=F32)
        for w in range(width):
            piece = both[:, w * 2 * orb : (w + 1) * 2 * orb]
            pieces.append(piece[:orb] + turned(piece[orb:]))
    return pieces


def first_modes(n, moves, extended, right, left):
    per, modes, _, wide = right.shape
    orb = wide // 2
    width = 2 if n % 2 == 0 else 1

    def kernel(moves, extended, right, left, *rest):
        outs, stack = rest[:n], rest[-1]
        me = lax.axis_index("eloc")
        even = lax.axis_index("egrp") & 1 == 0
        shifts = read_moves(moves, modes)
        places = {}
        for m in range(modes):
            for k in range(n):
                e = target_at(me, k, n) + n
                above, below = place_of(me, e + shifts[m], n), place_of(me, e - shifts[m], n)
                above = jnp.where(even & (above >= 2 * n), above - 2 * n, above)
                below = jnp.where(even & (below < n), below + 2 * n, below)
                places[m, k] = (above, below)
        for a in range(per):
            for m in range(modes):
                rows = [
                    jnp.concatenate([extended[places[m, k][0], a], extended[places[m, k][1], a]], 1)
                    for k in range(n)
                ]
                product = jnp.dot(jnp.concatenate(rows, 0), right[a, m], preferred_element_type=F32)
                put_products(stack, a, m, product.astype(BF16), n, width)
            for k, piece in enumerate(outer_products(stack, left, a, n, width)):
                outs[k][a] = piece

    return pl.pallas_call(
        kernel,
        name="first_modes",
        out_shape=[jax.ShapeDtypeStruct((per, orb, wide), F32) for _ in range(n)],
        in_specs=[VMEM for _ in range(4)],
        out_specs=[VMEM for _ in range(n)],
        scratch_shapes=[pltpu.VMEM((per, n // width, modes * orb, width * wide), BF16)],
        compiler_params=limited(),
        cost_estimate=cost(400_000_000),
    )(moves, extended, right, left)


def last_modes(n, groups, ks, moves, outer, partials, right, left):
    per, modes, _, wide = right.shape
    orb, count, late = wide // 2, len(ks), n - outer.shape[0]
    width = 2 if count % 2 == 0 else 1

    def kernel(moves, outer, right, left, *rest):
        partials, outs, (made, stack) = rest[:count], rest[count : 2 * count], rest[2 * count :]
        me = lax.axis_index("eloc")
        even = lax.axis_index("egrp") & 1 == 0
        group = lax.axis_index("egrp")
        within = (group > 0) & (group < groups - 1)
        begin = pl.multiple_of(jnp.where(even, wide, 0), wide)
        shifts = read_moves(moves, modes)
        places = {}
        for m in range(modes):
            for k in ks:
                e = target_at(me, k, n) + n
                t = jnp.where(even, e - shifts[m], e + shifts[m])
                outside = jnp.where(even, t < n, t >= 2 * n) & within
                base = jnp.where(even, 0, 2 * n)
                slot = jnp.where(outside, place_of(me, t, n) - base, 0)
                places[m, k] = (slot >= late, jnp.maximum(slot - late, 0))
        for a in range(per):
            blocks = jnp.concatenate([outer[b, a] for b in range(n - late)], 0)
            for m in range(0, modes, 2):
                both = [right[a, m + i, pl.ds(begin, wide)] for i in range(min(2, modes - m))]
                product = jnp.dot(blocks, jnp.concatenate(both, 1), preferred_element_type=F32).astype(BF16)
                for i in range(len(both)):
                    for b in range(n - late):
                        made[a, b, m + i] = product[b * orb : (b + 1) * orb, i * wide : (i + 1) * wide]
        for a in range(per):
            for m in range(modes):
                for q, k in enumerate(ks):
                    held, slot = places[m, k]
                    block = made[a, slot, m]
                    p, w = divmod(q, width)
                    stack[a, p, m * orb : (m + 1) * orb, w * wide : (w + 1) * wide] = jnp.where(
                        held, block, jnp.zeros_like(block)
                    )
        for a in range(per):
            for q, piece in enumerate(outer_products(stack, left, a, count, width)):
                outs[q][a] = (partials[q][a] + piece).astype(BF16)

    return pl.pallas_call(
        kernel,
        out_shape=[jax.ShapeDtypeStruct((per, orb, wide), BF16) for _ in ks],
        in_specs=[VMEM for _ in range(4 + count)],
        out_specs=[VMEM for _ in ks],
        scratch_shapes=[
            pltpu.VMEM((per, n - late, modes, orb, wide), BF16),
            pltpu.VMEM((per, count // width, modes * orb, width * wide), BF16),
        ],
        compiler_params=limited(),
        cost_estimate=cost(400_000_000),
    )(moves, outer, right, left, *[partials[k] for k in ks])


def joined(n, blocks):
    per, orb, wide = blocks[0].shape

    def kernel(*refs):
        blocks, out, done = refs[:n], refs[n], refs[n + 1]
        me = lax.axis_index("eloc")
        copies = []
        for k in range(n):
            place = out.at[0, pl.ds(source_at(me, k, n) * per, per)]
            copies.append(pltpu.make_async_copy(blocks[k], place, done.at[k]))
        for copy in copies:
            copy.start()
        for copy in copies:
            copy.wait()

    return pl.pallas_call(
        kernel,
        name="join",
        out_shape=jax.ShapeDtypeStruct((1, n * per, orb, wide), BF16),
        in_specs=[VMEM for _ in blocks],
        out_specs=HBM,
        scratch_shapes=[pltpu.SemaphoreType.DMA((n,))],
        compiler_params=limited(),
    )(*blocks)


def swapped(n, k, block):
    return lax.ppermute(block, "eloc", [(i, partner(i, k, n)) for i in range(n)])


def traded(groups, first, block):
    pairs = []
    for i in range(first, groups - 1 + (groups % 2 == 0) * first, 2):
        pairs += [(i, (i + 1) % groups), ((i + 1) % groups, i)]
    return lax.ppermute(block, "egrp", pairs)


def inside(groups, block):
    me = lax.axis_index("egrp")
    edge = (me == 0) | (me == groups - 1)
    return jnp.where(edge, jnp.zeros_like(block), block)


def shards(green_blocks, sigma_prev, neighbours, couplings, occupancy, shifts):
    n, groups = lax.axis_size("eloc"), lax.axis_size("egrp")
    per = couplings.shape[1]
    made = lesser_blocks(n, per, opened(), neighbours.T, green_blocks, sigma_prev)
    held = [made[0]] + [swapped(n, k, made[k]) for k in range(1, n)]
    right, left, moves = prepared(occupancy, shifts, couplings)
    soon = jnp.stack(held[: n // 2])
    early = traded(groups, 1, soon)
    here = jnp.stack(held)
    here, right, left, moves = lax.optimization_barrier((here, right, left, moves))
    outer = traded(groups, 1, jnp.stack(held[n // 2 :]))
    inner = traded(groups, 0, here)
    missing = jnp.zeros_like(outer)
    partials = first_modes(n, moves, jnp.concatenate([inner, here, inside(groups, early), missing], 0), right, left)
    back = {}
    for ks in (list(range(n)),):
        made = last_modes(n, groups, ks, moves, outer, partials, right, left)
        for k, block in zip(ks, made):
            back[k] = swapped(n, k, block) if k else block
    back = [back[k] for k in range(n)]
    return joined(n, back)


def solution(mesh):
    return jax.shard_map(
        shards,
        mesh=mesh,
        in_specs=(
            P(("egrp", "eloc"), None, None, None, None),
            P(("egrp", "eloc"), None, None, None),
            P(),
            P(None, "eloc", None, None),
            P(),
            P(),
        ),
        out_specs=P(("egrp", "eloc"), None, None, None),
        check_vma=False,
    )
```
